32 devices in a mesh: dp: 4 (over z), row: 2 (over y), col: 4 (over x, core).
Axes of the slice: x: 2, y: 2, z: 4, core: 2. Of those that a mesh axis runs over, the one named last changes fastest.
Arguments:
- activations: bfloat16 [4096, 4096], P('dp', 'col'), may hold values from -6 to 6
- out_grad: bfloat16 [4096, 14336], P('dp', 'row'), may hold values from -6 to 6
- weight: float32 [2, 7168, 4096], P('row', 'dp', 'col'), as said below
- step_size: float32 [2, 7168], P('row'), may hold values from 0.001 to 0.016
Outputs:
- input_grad: bfloat16 [4096, 4096], P(('dp', 'row'), 'col')
- weight_grad: float32 [2, 7168, 4096], P('row', 'dp', 'col')
- step_grad: float32 [2, 7168], P('row', 'dp')
The draws below stay inside these ranges and needn't reach their ends.
Inputs may be any that keep to these rules, and one draw needn't show every extreme that they name: Each latent weight divided by its row's step lies at least 0.1 away from every multiple of one half.
All inputs are finite; a program needn't handle non-finite values.
Results may differ from the reference program's by a relative error of at most 0.0096.
Values may be sent and summed in bfloat16 or wider, within the bound.
A program may use at most 128 MiB of HBM per device.

```python
import jax
import jax.numpy as jnp
from jax import lax

D = 4096
FF = 14336
TOKENS = 4096
N_ROW = 2


def joint_draw(key):
    base = jax.random.fold_in(key, 7)
    first, second, third, fourth = jax.random.split(base, 4)
    logs = jax.random.uniform(first, (N_ROW, FF // N_ROW), jnp.float32, jnp.log(0.002), jnp.log(0.008))
    scales = jnp.exp(logs)
    codes = jax.random.randint(second, (N_ROW, FF // N_ROW, D), -10, 10).astype(jnp.float32)
    magnitudes = jax.random.uniform(third, (N_ROW, FF // N_ROW, D), jnp.float32, 0.1, 0.4)
    signs = jnp.where(jax.random.bernoulli(fourth, 0.5, (N_ROW, FF // N_ROW, D)), 1.0, -1.0)
    latent = scales[:, :, None] * (codes + signs * magnitudes)
    return (scales, latent)


def draw_weight(key, part):
    scales, latent = joint_draw(key)
    return latent.astype(jnp.float32)


def draw_step_size(key, part):
    scales, latent = joint_draw(key)
    return scales.astype(jnp.float32)


def with_spikes(values, own_key, source, target, blocks, factor):
    owner, partner = [(jnp.arange(values.shape[position]) // (values.shape[position] // blocks)).reshape([-1 if axis == position else 1 for axis in range(values.ndim)]) for position in (source, target)]
    chosen = jax.random.permutation(own_key, blocks)[partner]
    strong = (owner == chosen) | (owner == (partner + blocks // 2) % blocks)
    return jnp.where(strong, factor * values, values)


def level_of(stream_key, shape, shards, smallest, top_value):
    def one(axis_at, shards_of):
        heights = jax.random.uniform(jax.random.fold_in(jax.random.fold_in(stream_key, 6), axis_at), (shards_of,), jnp.float32, smallest / len(shards), top_value / len(shards))
        return jnp.repeat(jnp.exp(heights), shape[axis_at] // shards_of).reshape((-1,) + (1,) * (len(shape) - axis_at - 1))

    level = one(*shards[0])
    for cut in shards[1:]:
        level = level * one(*cut)
    return level


def noise(key, dims, spread, bound, cuts=(), held_as=jnp.bfloat16):
    entries = jax.random.normal(key, dims, jnp.float32) * spread
    if len(cuts) > 0:
        entries = level_of(key, dims, cuts, -0.22, 0.18) * entries
    return jnp.clip(entries, min=-bound, max=bound).astype(held_as)


def heavy_noise(key, dims, spread, limit, shards, heavy, held_as=jnp.bfloat16):
    drawn = spread * jax.random.normal(key, dims, jnp.float32)
    if shards:
        drawn = drawn * level_of(key, dims, shards, -0.22, 0.18)
    return jnp.clip(with_spikes(drawn, jax.random.fold_in(key, 3), *heavy), -limit, limit).astype(held_as)


def setup_inputs(seed: int = 0) -> dict:
    arg_keys = jax.random.split(jax.random.key(seed), 5)
    activations = noise(arg_keys[0], (TOKENS, D), 1.0, 6.0, ((0, 4), (1, 4)))
    out_grad = heavy_noise(arg_keys[1], (TOKENS, FF), ((D / FF) ** 0.5), 6.0, ((0, 4), (1, 2)), (0, 1, 4, 2.0))
    weight = draw_weight(jax.random.fold_in(arg_keys[4], 71), 0)
    step_size = draw_step_size(jax.random.fold_in(arg_keys[4], 71), 0)
    return dict(activations=activations, out_grad=out_grad, weight=weight, step_size=step_size)


def reference(activations, out_grad, weight, step_size):
    scales = step_size.reshape(FF)
    latent = weight.reshape(FF, D)
    ratio = latent / scales[:, None]
    clipped = jnp.clip(ratio, -8.0, 7.0)
    levels = jnp.floor(clipped + 0.5)
    quantized = (levels * scales[:, None]).astype(jnp.bfloat16)
    inside = jnp.where((ratio >= -8.0) & (ratio <= 7.0), 1.0, 0.0).astype(jnp.float32)
    factor = jnp.where(inside > 0.5, levels - ratio, clipped)
    input_grad = jnp.dot(out_grad, quantized, preferred_element_type=jnp.float32).astype(jnp.bfloat16)
    products = lax.dot_general(out_grad, activations, (((0,), (0,)), ((), ())), preferred_element_type=jnp.float32)
    weight_grad = (products * inside).reshape(N_ROW, FF // N_ROW, D)
    grad_factor = 1.0 / (7.0 * D) ** 0.5
    step_grad = (jnp.sum(products * factor, axis=1) * grad_factor).reshape(N_ROW, FF // N_ROW)
    return input_grad, weight_grad, step_grad
```

```python
import jax
import jax.numpy as jnp
from jax import lax
from jax.sharding import PartitionSpec as P

D = 4096


def quantize(latent, scales):
    ratio = latent / scales[:, None]
    clipped = jnp.clip(ratio, -8.0, 7.0)
    levels = jnp.floor(clipped + 0.5)
    inside = jnp.where((ratio >= -8.0) & (ratio <= 7.0), 1.0, 0.0).astype(jnp.float32)
    factor = jnp.where(inside > 0.5, levels - ratio, clipped)
    quantized = (levels * scales[:, None]).astype(jnp.bfloat16)
    return (quantized, inside, factor)


def shift(block, axis, count, by):
    return lax.ppermute(block, axis, [(i, (i + by) % count) for i in range(count)])


def swap(block, axis, count, bit):
    return lax.ppermute(block, axis, [(i, i ^ bit) for i in range(count)])


def gather_rows(block, axis, count):
    position = lax.axis_index(axis)
    bit = 1
    bits = []
    while bit < count:
        bits.append(bit)
        bit *= 2
    pieces = {0: block}
    for bit in reversed(bits):
        held = dict(pieces)
        for key in held:
            pieces[key ^ bit] = swap(held[key], axis, count, bit)
    parts = [pieces[key] for key in range(count)]
    for bit in bits:
        flag = (position & bit) != 0
        parts = [
            jnp.where(flag, parts[key ^ bit], parts[key]) for key in range(count)
        ]
    return jnp.concatenate(parts, axis=0)


def make_shards(n_dp, n_row, n_col):
    def shards(activations, out_grad, weight, step_size):
        own_count = weight.shape[1]
        tokens = out_grad.shape[0]
        dp = lax.axis_index("dp")
        row = lax.axis_index("row")
        col = lax.axis_index("col")
        scales = step_size[0]
        own_scales = lax.dynamic_slice_in_dim(scales, dp * own_count, own_count, 0)
        grad_factor = 1.0 / (7.0 * D) ** 0.5

        share = tokens // n_col
        half = tokens // n_row
        mine = lax.dynamic_slice_in_dim(out_grad, col * share, share, 0)
        ring = lax.dynamic_slice_in_dim(activations, row * half, half, 0)
        grads, acts = [], []
        for k in range(1, n_dp):
            target = (dp + k) % n_dp
            chunk = lax.dynamic_slice_in_dim(mine, target * own_count, own_count, 1)
            grads.append(shift(chunk, "dp", n_dp, k))
            ring = shift(ring, "dp", n_dp, 1)
            acts.append(ring)

        quantized, inside, factor = quantize(weight[0], own_scales)
        own_grad = lax.dynamic_slice_in_dim(out_grad, dp * own_count, own_count, 1)

        def reduced(grad):
            size = tokens
            bit = n_row // 2
            if bit == 0:
                return jnp.dot(grad, quantized, preferred_element_type=jnp.float32)
            size //= 2
            upper = ((row // bit) % 2).astype(jnp.int32)
            sent = lax.dynamic_slice_in_dim(grad, (1 - upper) * size, size, 0)
            kept = lax.dynamic_slice_in_dim(grad, upper * size, size, 0)
            out = jnp.dot(sent, quantized, preferred_element_type=jnp.float32).astype(jnp.bfloat16)
            came = swap(out, "row", n_row, bit)
            total = jnp.dot(kept, quantized, preferred_element_type=jnp.float32) + came.astype(jnp.float32)
            bit //= 2
            while bit:
                size //= 2
                upper = (row // bit) % 2 == 1
                low, high = total[:size], total[size:]
                came = swap(jnp.where(upper, low, high).astype(jnp.bfloat16), "row", n_row, bit)
                total = jnp.where(upper, high, low) + came.astype(jnp.float32)
                bit //= 2
            return total

        products = lax.dot_general(
            own_grad, activations, (((0,), (0,)), ((), ())), preferred_element_type=jnp.float32
        )
        own_total = reduced(own_grad)
        running = None
        for k in range(1, n_dp):
            grad = gather_rows(grads[k - 1], "col", n_col)
            total = reduced(grad)
            if running is not None:
                total = total + running.astype(jnp.float32)
            running = shift(total.astype(jnp.bfloat16), "dp", n_dp, 1)
            act = gather_rows(acts[k - 1], "row", n_row)
            products = products + lax.dot_general(
                grad, act, (((0,), (0,)), ((), ())), preferred_element_type=jnp.float32
            )
        if running is not None:
            own_total = own_total + running.astype(jnp.float32)
        input_grad = own_total.astype(jnp.bfloat16)
        step_rows = lax.psum(jnp.sum(products * factor, axis=1) * grad_factor, "col")
        weight_grad = (products * inside)[None]
        return (input_grad, weight_grad, step_rows[None])

    return shards


def solution(mesh):
    in_specs = (P("dp", "col"), P("dp", "row"), P("row", "dp", "col"), P("row", None))
    out_specs = (P(("dp", "row"), "col"), P("row", "dp", "col"), P("row", "dp"))
    shards = make_shards(mesh.shape["dp"], mesh.shape["row"], mesh.shape["col"])
    return jax.shard_map(shards, mesh=mesh, in_specs=in_specs, out_specs=out_specs, check_vma=False)
```

```python
import jax
import jax.numpy as jnp
from jax import lax
from jax.experimental.layout import Layout, with_layout_constraint
from jax.sharding import PartitionSpec as P

D = 4096


def quantize(latent, scales):
    ratio = latent / scales[:, None]
    clipped = jnp.clip(ratio, -8.0, 7.0)
    levels = jnp.floor(clipped + 0.5)
    inside = jnp.where((ratio >= -8.0) & (ratio <= 7.0), 1.0, 0.0).astype(jnp.float32)
    factor = jnp.where(inside > 0.5, levels - ratio, clipped)
    quantized = (levels * scales[:, None]).astype(jnp.bfloat16)
    return (quantized, inside, factor)


def shift(block, axis, count, by):
    return lax.ppermute(block, axis, [(i, (i + by) % count) for i in range(count)])


def swap(block, axis, count, bit):
    return lax.ppermute(block, axis, [(i, i ^ bit) for i in range(count)])


def gather_rows(block, axis, count):
    position = lax.axis_index(axis)
    bit = 1
    bits = []
    while bit < count:
        bits.append(bit)
        bit *= 2
    pieces = {0: block}
    for bit in reversed(bits):
        held = dict(pieces)
        for key in held:
            pieces[key ^ bit] = swap(held[key], axis, count, bit)
    parts = [pieces[key] for key in range(count)]
    for bit in bits:
        flag = (position & bit) != 0
        parts = [
            jnp.where(flag, parts[key ^ bit], parts[key]) for key in range(count)
        ]
    return jnp.concatenate(parts, axis=0)


def make_shards(n_dp, n_row, n_col):
    def shards(activations, out_grad, weight, step_size):
        own_count = weight.shape[1]
        tokens = out_grad.shape[0]
        dp = lax.axis_index("dp")
        row = lax.axis_index("row")
        col = lax.axis_index("col")
        scales = step_size[0]
        own_scales = lax.dynamic_slice_in_dim(scales, dp * own_count, own_count, 0)
        grad_factor = 1.0 / (7.0 * D) ** 0.5

        share = tokens // n_col
        half = tokens // n_row
        mine = lax.dynamic_slice_in_dim(out_grad, col * share, share, 0)
        ring = lax.dynamic_slice_in_dim(activations, row * half, half, 0)
        grads, acts = [], []
        for k in range(1, n_dp):
            target = (dp + k) % n_dp
            chunk = lax.dynamic_slice_in_dim(mine, target * own_count, own_count, 1)
            grads.append(shift(chunk, "dp", n_dp, k))
            ring = shift(ring, "dp", n_dp, 1)
            acts.append(ring)

        quantized, _, _ = quantize(weight[0], own_scales)
        own_grad = lax.dynamic_slice_in_dim(out_grad, dp * own_count, own_count, 1)

        def reduced(grad):
            size = tokens
            bit = n_row // 2
            if bit == 0:
                return jnp.dot(grad, quantized, preferred_element_type=jnp.float32)
            size //= 2
            upper = ((row // bit) % 2).astype(jnp.int32)
            sent = lax.dynamic_slice_in_dim(grad, (1 - upper) * size, size, 0)
            kept = lax.dynamic_slice_in_dim(grad, upper * size, size, 0)
            out = jnp.dot(sent, quantized, preferred_element_type=jnp.float32).astype(jnp.bfloat16)
            came = swap(out, "row", n_row, bit)
            total = jnp.dot(kept, quantized, preferred_element_type=jnp.float32) + came.astype(jnp.float32)
            bit //= 2
            while bit:
                size //= 2
                upper = (row // bit) % 2 == 1
                low, high = total[:size], total[size:]
                came = swap(jnp.where(upper, low, high).astype(jnp.bfloat16), "row", n_row, bit)
                total = jnp.where(upper, high, low) + came.astype(jnp.float32)
                bit //= 2
            return total

        products = lax.dot_general(
            own_grad, activations, (((0,), (0,)), ((), ())), preferred_element_type=jnp.float32
        )
        own_total = reduced(own_grad)
        if grads:
            grads[0], quantized, products = lax.optimization_barrier((grads[0], quantized, products))
        running = None
        for k in range(1, n_dp):
            grad = gather_rows(grads[k - 1], "col", n_col)
            total = reduced(grad)
            if running is not None:
                total = total + running.astype(jnp.float32)
            leaving, grad = lax.optimization_barrier((total.astype(jnp.bfloat16), grad))
            running = shift(leaving, "dp", n_dp, 1)
            act = gather_rows(acts[k - 1], "row", n_row)
            products = products + lax.dot_general(
                grad, act, (((0,), (0,)), ((), ())), preferred_element_type=jnp.float32
            )
        if running is not None:
            own_total = own_total + running.astype(jnp.float32)
        products, latent = lax.optimization_barrier((products, weight[0]))
        products = with_layout_constraint(products, Layout((0, 1)))
        _, inside, factor = quantize(latent, own_scales)
        input_grad = own_total.astype(jnp.bfloat16)
        step_rows = lax.psum(jnp.sum(products * factor, axis=1) * grad_factor, "col")
        weight_grad = (products * inside)[None]
        return (input_grad, weight_grad, step_rows[None])

    return shards


def solution(mesh):
    in_specs = (P("dp", "col"), P("dp", "row"), P("row", "dp", "col"), P("row", None))
    out_specs = (P(("dp", "row"), "col"), P("row", "dp", "col"), P("row", "dp"))
    shards = make_shards(mesh.shape["dp"], mesh.shape["row"], mesh.shape["col"])
    return jax.shard_map(shards, mesh=mesh, in_specs=in_specs, out_specs=out_specs, check_vma=False)
```
